32 devices in a mesh: grid: 8 (over y, x, core), band: 4 (over z).
Axes of the slice: x: 2, y: 2, z: 4, core: 2. Of those that a mesh axis runs over, the one named last changes fastest.
Arguments:
- orbitals: bfloat16 [32, 64, 64, 128], P('band', 'grid'), may hold values from -6 to 6
- occupation: int32 [32], P('band'), may hold values from 1 to 2
- spin_of_band: int32 [32], P('band'), may hold values from 0 to 1
- ionic_charge: float32 [64, 64, 128], P('grid'), may hold values from 0.3 to 3
Outputs:
- potential: float32 [2, 64, 64, 128], P(None, 'grid')
- applied: bfloat16 [32, 64, 64, 128], P('band', 'grid')
The draws below stay inside these ranges and needn't reach their ends.
All inputs are finite; a program needn't handle non-finite values.
Results may differ from the reference program's by a relative error of at most 0.001.
Values sent between devices are 32-bit elements; how exact they have to be, the bound alone decides.
A program may use at most 64 MiB of HBM per device.

```python
import math
import jax
import jax.numpy as jnp
from jax import lax

NX = 128
NY = 64
NZ = 64
BANDS = 32


def with_ends(entries, rng, smallest, largest):
    shape = entries.shape
    spot = [jax.random.randint(jax.random.fold_in(rng, axis), (), 0, shape[axis]) for axis in range(len(shape))]
    entries = entries.at[tuple(spot)].set(smallest)
    longest = shape.index(max(shape))
    spot[longest] = (spot[longest] + 1) % shape[longest]
    return entries.at[tuple(spot)].set(largest)


def block_levels(stream_key, dims, shards, low, high):
    def one(position, parts):
        draws = jax.random.uniform(jax.random.fold_in(jax.random.fold_in(stream_key, 6), position), (parts,), jnp.float32, low / len(shards), high / len(shards))
        return jnp.repeat(jnp.exp(draws), dims[position] // parts).reshape((-1,) + (1,) * (len(dims) - position - 1))

    level = one(*shards[0])
    for cut in shards[1:]:
        level = level * one(*cut)
    return level


def noise(rng, extent, width, most, pieces=(), kind=jnp.bfloat16):
    entries = jax.random.normal(rng, extent, jnp.float32) * width
    if len(pieces) > 0:
        entries = block_levels(rng, extent, pieces, -0.22, 0.18) * entries
    return jnp.clip(entries, min=-most, max=most).astype(kind)


def setup_inputs(seed: int = 0) -> dict:
    key_of = jax.random.split(jax.random.key(seed), 5)
    return {
        "orbitals": noise(key_of[0], (BANDS, NZ, NY, NX), 1.0, 6.0, ((0, 4), (1, 8))),
        "occupation": with_ends(jax.random.randint(key_of[1], (BANDS,), 1, 3), jax.random.fold_in(key_of[1], 1), 1, 2).astype(jnp.int32),
        "spin_of_band": with_ends(jax.random.randint(key_of[2], (BANDS,), 0, 2), jax.random.fold_in(key_of[2], 1), 0, 1).astype(jnp.int32),
        "ionic_charge": jnp.clip(jnp.exp(math.log(3.0) - 2.3025851 * jax.random.uniform(key_of[3], (NZ, NY, NX), jnp.float32) ** block_levels(key_of[3], (NZ, NY, NX), ((0, 8),), -0.2, 0.2)), 0.3, 3.0),
    }


spacing = 0.25


def signed_sq(count):
    index = jnp.arange(count, dtype=jnp.int32)
    signed = jnp.where(index < count // 2, index, index - count).astype(jnp.float32)
    wave = 2.0 * math.pi * signed / (count * spacing)
    return wave * wave


def reference(orbitals, occupation, spin_of_band, ionic_charge):
    total = orbitals.shape[0]
    channels = jnp.arange(2, dtype=jnp.int32)
    weights = jnp.where(spin_of_band[None, :] == channels[:, None], occupation[None, :].astype(jnp.float32), jnp.float32(0.0)) / total

    def accumulate(acc, pair):
        column, orbital = pair
        square = orbital.astype(jnp.float32) * orbital.astype(jnp.float32)
        return acc + column[:, None, None, None] * square[None], None

    start = jnp.zeros((2,) + orbitals.shape[1:], jnp.float32)
    density, unused = lax.scan(accumulate, start, (weights.T, orbitals))
    exchange = -jnp.cbrt(6.0 / math.pi * density)
    net = density[0] + density[1] - ionic_charge
    nz, ny, nx = net.shape
    g_sq = signed_sq(nz)[:, None, None] + signed_sq(ny)[None, :, None] + signed_sq(nx)[None, None, :]
    kernel = jnp.where(g_sq > 0, 4.0 * math.pi / jnp.where(g_sq > 0, g_sq, 1.0), 0.0)
    hartree = jnp.real(jnp.fft.ifftn(jnp.fft.fftn(net) * kernel)).astype(jnp.float32)
    potential = hartree[None] + exchange

    def apply_one(pair):
        channel, orbital = pair
        return (potential[channel] * orbital.astype(jnp.float32)).astype(jnp.bfloat16)

    applied = lax.map(apply_one, (spin_of_band, orbitals))
    return potential, applied
```

```python
import functools
import math

import jax
import jax.numpy as jnp
import numpy as np
from jax import lax
from jax.experimental import pallas as pl
from jax.experimental.pallas import tpu as pltpu
from jax.sharding import PartitionSpec as P

spacing = 0.25
highest = lax.Precision.HIGHEST


def tables(count):
    index = jnp.arange(count, dtype=jnp.int32)
    product = index[:, None] * index[None, :] % count
    angle = 2.0 * math.pi * product.astype(jnp.float32) / count
    return (jnp.cos(angle), jnp.sin(angle))


def signed_sq(index, count):
    signed = jnp.where(index < count // 2, index, index - count).astype(jnp.float32)
    wave = 2.0 * math.pi * signed / (count * spacing)
    return wave * wave


def kernel_at(depth, row_index, rows, col_index, cols):
    g_sq = signed_sq(jnp.arange(depth, dtype=jnp.int32), depth)[:, None, None]
    g_sq = g_sq + signed_sq(row_index, rows)[None, :, None]
    g_sq = g_sq + signed_sq(col_index, cols)[None, None, :]
    return jnp.where(g_sq > 0, 4.0 * math.pi / jnp.where(g_sq > 0, g_sq, 1.0), 0.0)


def along(table, field, form):
    return jnp.einsum(form, table, field, precision=highest)


def forward_y(cos_y, sin_y, real_x, imag_x):
    form_y = "ky,zyx->zkx"
    real_y = along(cos_y, real_x, form_y) + along(sin_y, imag_x, form_y)
    imag_y = along(cos_y, imag_x, form_y) - along(sin_y, real_x, form_y)
    return (real_y, imag_y)


def inverse_y(cos_y, sin_y, real_k, imag_k):
    form_y = "ky,zyx->zkx"
    plane_real = along(cos_y, real_k, form_y) - along(sin_y, imag_k, form_y)
    plane_imag = along(cos_y, imag_k, form_y) + along(sin_y, real_k, form_y)
    return (plane_real, plane_imag)


def z_kernel(cos_z, sin_z, moved, kernel):
    form_z = "kz,zyx->kyx"
    real_z = along(cos_z, moved[0], form_z) + along(sin_z, moved[1], form_z)
    imag_z = along(cos_z, moved[1], form_z) - along(sin_z, moved[0], form_z)
    real_k = real_z * kernel
    imag_k = imag_z * kernel
    back_real = along(cos_z, real_k, form_z) - along(sin_z, imag_k, form_z)
    back_imag = along(cos_z, imag_k, form_z) + along(sin_z, real_k, form_z)
    return jnp.stack([back_real, back_imag])


def solve_hartree(net, depth):
    planes, rows, cols = net.shape
    cos_x, sin_x = tables(cols)
    cos_y, sin_y = tables(rows)
    cos_z, sin_z = tables(depth)
    local_rows = rows // lax.axis_size("grid")
    row_index = lax.axis_index("grid") * local_rows + jnp.arange(local_rows, dtype=jnp.int32)
    real_x = jnp.dot(net, cos_x, precision=highest)
    imag_x = -jnp.dot(net, sin_x, precision=highest)
    real_y, imag_y = forward_y(cos_y, sin_y, real_x, imag_x)
    moved = lax.all_to_all(
        jnp.stack([real_y, imag_y]), "grid", split_axis=2, concat_axis=1, tiled=True
    )
    kernel = kernel_at(depth, row_index, rows, jnp.arange(cols, dtype=jnp.int32), cols)
    back = z_kernel(cos_z, sin_z, moved, kernel)
    returned = lax.all_to_all(back, "grid", split_axis=1, concat_axis=2, tiled=True)
    plane_real, plane_imag = inverse_y(cos_y, sin_y, returned[0], returned[1])
    result = jnp.dot(plane_real, cos_x, precision=highest) - jnp.dot(
        plane_imag, sin_x, precision=highest
    )
    return result / (cols * rows * depth)


def local(ng, orbitals, occupation, spin_of_band, ionic_charge):
    bands, planes, rows, cols = orbitals.shape
    total = bands * lax.axis_size("band")
    channels = jnp.arange(2, dtype=jnp.int32)
    weights = (
        jnp.where(
            spin_of_band[None, :] == channels[:, None], occupation[None, :].astype(jnp.float32), 0.0
        )
        / total
    )
    values = orbitals.astype(jnp.float32)
    squares = (values * values).reshape(bands, -1)
    partial_value = jnp.dot(weights, squares, precision=highest).reshape(2, planes, rows, cols)
    share = lax.psum_scatter(partial_value, "band", scatter_dimension=2, tiled=True)
    share_rows = share.shape[2]
    ion_share = lax.dynamic_slice_in_dim(
        ionic_charge, lax.axis_index("band") * share_rows, share_rows, 1
    )
    fields = jnp.concatenate(
        [-jnp.cbrt(6.0 / math.pi * share), (share[0] + share[1] - ion_share)[None]], 0
    )
    whole = lax.all_gather(fields, "band", axis=2, tiled=True)
    potential = solve_hartree(whole[2], planes * ng)[None] + whole[:2]
    pick = (spin_of_band[:, None] == channels[None, :]).astype(jnp.float32)
    chosen = jnp.dot(pick, potential.reshape(2, -1), precision=highest).reshape(
        bands, planes, rows, cols
    )
    applied = (chosen * values).astype(jnp.bfloat16)
    return (potential, applied)

MESH = pl.DeviceIdType.MESH
f32 = jnp.float32
bf16 = jnp.bfloat16


def cas_table(count):
    product = np.outer(np.arange(count), np.arange(count)) % count
    angle = 2.0 * math.pi * product / count
    return (np.cos(angle) + np.sin(angle)) / math.sqrt(count)


def parts_of(table):
    high = table.astype(np.float32).astype(bf16)
    low = (table - high.astype(np.float64)).astype(np.float32).astype(bf16)
    return high, low


def right_table(count):
    high, low = parts_of(cas_table(count))
    return np.concatenate([high, high, low], 0)


def left_table(count):
    high, low = parts_of(cas_table(count))
    return np.concatenate([high, low, high], 1)


def two_parts(value):
    high = value.astype(bf16)
    low = (value - high.astype(f32)).astype(bf16)
    return high, low


def right_mul(value, table):
    high, low = two_parts(value)
    return jnp.dot(jnp.concatenate([high, low, high], 1), table, preferred_element_type=f32)


def left_mul(table, value):
    high, low = two_parts(value)
    return jnp.dot(table, jnp.concatenate([high, high, low], 0), preferred_element_type=f32)


def cube_root(value):
    safe = jnp.where(value > 0, value, 1.0)
    return jnp.where(value > 0, jnp.exp(jnp.log(safe) * (1.0 / 3.0)), 0.0)


def wave_sq(index, count):
    signed = jnp.where(index < count // 2, index, index - count).astype(f32)
    wave = signed * (2.0 * math.pi / (count * spacing))
    return wave * wave


def field_kernel(
    ng, nb, lag,
    occ, spin, orb_hbm, ion_hbm, hx_hbm, hy_hbm, hz_hbm,
    pot,
    orb, ion, hx, hy, hz, part, near_in, near_out, far_in, far_out, ex,
    y_out, z_in, z_out, y_in,
    orb_sem, in_sem, near_s, near_r, far_s, far_r, fwd_s, fwd_r, back_s, back_r,
):
    bands, planes, rows, cols = orb.shape
    depth = planes * ng
    lines = rows // ng
    g = lax.axis_index("grid")
    i = lax.axis_index("band")
    side = (2 * i) // nb
    inner = jnp.logical_and(i > 0, i < nb - 1)
    inward = i + 1 - 2 * side
    outward = jnp.clip(i - 1 + 2 * side, 0, nb - 1)

    barrier = pltpu.get_barrier_semaphore()
    for k in range(1, ng):
        pl.semaphore_signal(barrier, inc=1, device_id={"grid": lax.rem(g + k, ng)}, device_id_type=MESH)
    pl.semaphore_signal(barrier, inc=1, device_id={"band": inward}, device_id_type=MESH)

    @pl.when(inner)
    def _():
        pl.semaphore_signal(barrier, inc=1, device_id={"band": outward}, device_id_type=MESH)

    loads = []
    for p in range(planes):
        copy = pltpu.make_async_copy(orb_hbm.at[:, p], orb.at[:, p], orb_sem.at[p])
        copy.start()
        loads.append(copy)
    others = []
    for k, (src, dst) in enumerate(((ion_hbm, ion), (hx_hbm, hx), (hy_hbm, hy), (hz_hbm, hz))):
        copy = pltpu.make_async_copy(src, dst, in_sem.at[k])
        copy.start()
        others.append(copy)

    scale = 1.0 / (bands * nb)
    up = [occ[b].astype(f32) * spin[b].astype(f32) * scale for b in range(bands)]
    down = [occ[b].astype(f32) * (1 - spin[b]).astype(f32) * scale for b in range(bands)]

    def near_copy(p):
        return pltpu.make_async_remote_copy(
            src_ref=near_out.at[p], dst_ref=far_in.at[p],
            send_sem=near_s.at[p], recv_sem=far_r.at[p],
            device_id={"band": inward}, device_id_type=MESH,
        )

    def crossing(p):
        return pltpu.make_async_remote_copy(
            src_ref=near_out.at[p], dst_ref=near_in.at[p],
            send_sem=near_s.at[p], recv_sem=near_r.at[p],
            device_id={"band": inward}, device_id_type=MESH,
        )

    def far_copy(p):
        return pltpu.make_async_remote_copy(
            src_ref=far_out.at[p], dst_ref=far_in.at[p],
            send_sem=far_s.at[p], recv_sem=far_r.at[p],
            device_id={"band": outward}, device_id_type=MESH,
        )

    middle = jnp.where(side == 0, i + 1 == nb // 2, i == nb // 2)

    def send_near(p):
        @pl.when(middle)
        def _():
            near_copy(p).start()

        @pl.when(jnp.logical_not(middle))
        def _():
            crossing(p).start()

    def density(p):
        loads[p].wait()
        zero = one = None
        for b in range(bands):
            value = orb[b, p].astype(f32)
            square = value * value
            zero = down[b] * square if b == 0 else zero + down[b] * square
            one = up[b] * square if b == 0 else one + up[b] * square
        return zero, one

    def near_step(p):
        @pl.when(inner)
        def _():
            near_r_wait = crossing(p)
            near_r_wait.wait_recv()
            near_out[p] = part[p] + near_in[p]

        @pl.when(inner)
        def _():
            send_near(p)

    def fwd_copy(p, k):
        target = lax.rem(g + k, ng)
        return pltpu.make_async_remote_copy(
            src_ref=y_out.at[target, pl.ds(p * lines, lines)],
            dst_ref=z_in.at[pl.ds(pl.multiple_of((g * planes + p) * lines, lines), lines)],
            send_sem=fwd_s.at[p, k], recv_sem=fwd_r.at[p, k],
            device_id={"grid": target}, device_id_type=MESH,
        )

    def far_step(p):
        far_copy(p).wait_recv()

        @pl.when(inner)
        def _():
            far_out[p] = part[p] + far_in[p]
            far_copy(p).start()

        zero = near_out[p, 0] + far_in[p, 0]
        one = near_out[p, 1] + far_in[p, 1]
        net = zero + one - ion[p]
        spectrum = left_mul(hy[...], right_mul(net, hx[...]))
        for t in range(ng):
            y_out[t, pl.ds(p * lines, lines)] = spectrum[t * lines:(t + 1) * lines]
        for k in range(1, ng):
            fwd_copy(p, k).start()
        z_in[pl.ds(pl.multiple_of((g * planes + p) * lines, lines), lines)] = y_out[g, pl.ds(p * lines, lines)]
        ex[0, p] = -cube_root(zero * (6.0 / math.pi))
        ex[1, p] = -cube_root(one * (6.0 / math.pi))

    for p in range(planes):
        zero, one = density(p)
        part[p, 0] = zero
        part[p, 1] = one

        @pl.when(jnp.logical_not(inner))
        def _():
            near_out[p, 0] = zero
            near_out[p, 1] = one

        if p == 0:
            pl.semaphore_wait(barrier, ng + jnp.where(inner, 1, 0))

        @pl.when(jnp.logical_not(inner))
        def _():
            send_near(p)

    for copy in others:
        copy.wait()
    for step in range(planes + lag):
        if step < planes:
            near_step(step)
        if step >= lag:
            far_step(step - lag)

    kz = lax.broadcasted_iota(jnp.int32, (depth, cols), 0)
    kx = lax.broadcasted_iota(jnp.int32, (depth, cols), 1)
    flat = wave_sq(kz, depth) + wave_sq(kx, cols)

    def kernel_of(line):
        total = flat + wave_sq(g * lines + line, rows)
        return jnp.where(total > 0, 4.0 * math.pi / jnp.where(total > 0, total, 1.0), 0.0)

    for p in range(planes):
        for k in range(1, ng):
            fwd_copy(p, k).wait_recv()

    group = 2

    def back_copy(start, k):
        target = lax.rem(g + k, ng)
        return pltpu.make_async_remote_copy(
            src_ref=z_out.at[target, pl.ds(start * planes, group * planes)],
            dst_ref=y_in.at[pl.ds(pl.multiple_of((g * lines + start) * planes, group * planes), group * planes)],
            send_sem=back_s.at[start // group, k], recv_sem=back_r.at[start // group, k],
            device_id={"grid": target}, device_id_type=MESH,
        )

    for start in range(0, lines, group):
        picked = [z_in[pl.ds(start + t, depth, stride=lines), :] for t in range(group)]
        weights = jnp.concatenate([kernel_of(start + t) for t in range(group)], 1)
        waves = left_mul(hz[...], jnp.concatenate(picked, 1))
        field = left_mul(hz[...], waves * weights)
        for t in range(group):
            for d in range(ng):
                z_out[d, pl.ds((start + t) * planes, planes)] = field[
                    d * planes:(d + 1) * planes, t * cols:(t + 1) * cols
                ]
        for k in range(1, ng):
            back_copy(start, k).start()
        y_in[pl.ds(pl.multiple_of((g * lines + start) * planes, group * planes), group * planes)] = z_out[
            g, pl.ds(start * planes, group * planes)
        ]

    for start in range(0, lines, group):
        for k in range(1, ng):
            back_copy(start, k).wait_recv()

    for p in range(0, planes, 2):
        picked = [y_in[pl.ds(p + t, rows, stride=planes), :] for t in range(2)]
        mixed = left_mul(hy[...], jnp.concatenate(picked, 1))
        both = right_mul(jnp.concatenate([mixed[:, :cols], mixed[:, cols:]], 0), hx[...])
        for t in range(2):
            hartree = both[t * rows:(t + 1) * rows]
            pot[0, p + t] = hartree + ex[0, p + t]
            pot[1, p + t] = hartree + ex[1, p + t]

    for p in range(planes):
        near_copy(p).wait_send()

        @pl.when(inner)
        def _():
            far_copy(p).wait_send()

        for k in range(1, ng):
            fwd_copy(p, k).wait_send()
    for start in range(0, lines, group):
        for k in range(1, ng):
            back_copy(start, k).wait_send()


def apply_kernel(spin, pot_in, orb, pot, out):
    pot[...] = pot_in[...]
    for b in range(orb.shape[0]):
        chosen = jnp.where(spin[b] == 1, pot_in[1], pot_in[0])
        out[b] = (chosen * orb[b].astype(f32)).astype(bf16)


def fast(ng, nb, orbitals, occupation, spin_of_band, ionic_charge):
    bands, planes, rows, cols = orbitals.shape
    depth = planes * ng
    lines = rows // ng
    lag = 2
    dma = pltpu.SemaphoreType.DMA
    field = (planes, 2, rows, cols)
    anywhere = pl.BlockSpec(memory_space=pl.ANY)
    scalar = pl.BlockSpec(memory_space=pltpu.SMEM)
    potential = pl.pallas_call(
        functools.partial(field_kernel, ng, nb, lag),
        name="fields",
        out_shape=jax.ShapeDtypeStruct((2, planes, rows, cols), f32),
        in_specs=[scalar, scalar] + [anywhere] * 5,
        out_specs=pl.BlockSpec(memory_space=pltpu.VMEM),
        scratch_shapes=[
            pltpu.VMEM(orbitals.shape, bf16),
            pltpu.VMEM((planes, rows, cols), f32),
            pltpu.VMEM((3 * cols, cols), bf16),
            pltpu.VMEM((rows, 3 * rows), bf16),
            pltpu.VMEM((depth, 3 * depth), bf16),
            pltpu.VMEM(field, f32),
            pltpu.VMEM(field, f32),
            pltpu.VMEM(field, f32),
            pltpu.VMEM(field, f32),
            pltpu.VMEM(field, f32),
            pltpu.VMEM((2, planes, rows, cols), f32),
            pltpu.VMEM((ng, planes * lines, cols), f32),
            pltpu.VMEM((depth * lines, cols), f32),
            pltpu.VMEM((ng, planes * lines, cols), f32),
            pltpu.VMEM((rows * planes, cols), f32),
            dma((planes,)),
            dma((4,)),
            dma((planes,)),
            dma((planes,)),
            dma((planes,)),
            dma((planes,)),
            dma((planes, ng)),
            dma((planes, ng)),
            dma((lines // 2, ng)),
            dma((lines // 2, ng)),
        ],
        compiler_params=pltpu.CompilerParams(
            collective_id=0, has_side_effects=True, vmem_limit_bytes=32 * 1024 * 1024
        ),
    )(
        occupation, spin_of_band, orbitals, ionic_charge,
        jnp.asarray(right_table(cols)), jnp.asarray(left_table(rows)), jnp.asarray(left_table(depth)),
    )
    step = 2
    return pl.pallas_call(
        apply_kernel,
        name="apply",
        grid=(planes // step,),
        out_shape=(
            jax.ShapeDtypeStruct(potential.shape, f32),
            jax.ShapeDtypeStruct(orbitals.shape, bf16),
        ),
        in_specs=[
            scalar,
            pl.BlockSpec((2, step, rows, cols), lambda p: (0, p, 0, 0)),
            pl.BlockSpec((bands, step, rows, cols), lambda p: (0, p, 0, 0)),
        ],
        out_specs=(
            pl.BlockSpec((2, step, rows, cols), lambda p: (0, p, 0, 0)),
            pl.BlockSpec((bands, step, rows, cols), lambda p: (0, p, 0, 0)),
        ),
    )(spin_of_band, potential, orbitals)


def solution(mesh):
    ng, nb = mesh.shape["grid"], mesh.shape["band"]

    def body(orbitals, occupation, spin_of_band, ionic_charge):
        bands, planes, rows, cols = orbitals.shape
        lines = rows // ng
        suits = planes % 8 == 0 and lines % 8 == 0 and rows % 16 == 0
        if suits and cols % 128 == 0 and nb % 2 == 0 and ng > 1:
            return fast(ng, nb, orbitals, occupation, spin_of_band, ionic_charge)
        return local(ng, orbitals, occupation, spin_of_band, ionic_charge)

    return jax.shard_map(
        body,
        mesh=mesh,
        in_specs=(P("band", "grid", None, None), P("band"), P("band"), P("grid", None, None)),
        out_specs=(P(None, "grid", None, None), P("band", "grid", None, None)),
        check_vma=False,
    )
```

```python
import functools
import math

import jax
import jax.numpy as jnp
import numpy as np
from jax import lax
from jax.experimental import pallas as pl
from jax.experimental.pallas import tpu as pltpu
from jax.sharding import PartitionSpec as P

spacing = 0.25
highest = lax.Precision.HIGHEST


def tables(count):
    index = jnp.arange(count, dtype=jnp.int32)
    product = index[:, None] * index[None, :] % count
    angle = 2.0 * math.pi * product.astype(jnp.float32) / count
    return (jnp.cos(angle), jnp.sin(angle))


def signed_sq(index, count):
    signed = jnp.where(index < count // 2, index, index - count).astype(jnp.float32)
    wave = 2.0 * math.pi * signed / (count * spacing)
    return wave * wave


def kernel_at(depth, row_index, rows, col_index, cols):
    g_sq = signed_sq(jnp.arange(depth, dtype=jnp.int32), depth)[:, None, None]
    g_sq = g_sq + signed_sq(row_index, rows)[None, :, None]
    g_sq = g_sq + signed_sq(col_index, cols)[None, None, :]
    return jnp.where(g_sq > 0, 4.0 * math.pi / jnp.where(g_sq > 0, g_sq, 1.0), 0.0)


def along(table, field, form):
    return jnp.einsum(form, table, field, precision=highest)


def forward_y(cos_y, sin_y, real_x, imag_x):
    form_y = "ky,zyx->zkx"
    real_y = along(cos_y, real_x, form_y) + along(sin_y, imag_x, form_y)
    imag_y = along(cos_y, imag_x, form_y) - along(sin_y, real_x, form_y)
    return (real_y, imag_y)


def inverse_y(cos_y, sin_y, real_k, imag_k):
    form_y = "ky,zyx->zkx"
    plane_real = along(cos_y, real_k, form_y) - along(sin_y, imag_k, form_y)
    plane_imag = along(cos_y, imag_k, form_y) + along(sin_y, real_k, form_y)
    return (plane_real, plane_imag)


def z_kernel(cos_z, sin_z, moved, kernel):
    form_z = "kz,zyx->kyx"
    real_z = along(cos_z, moved[0], form_z) + along(sin_z, moved[1], form_z)
    imag_z = along(cos_z, moved[1], form_z) - along(sin_z, moved[0], form_z)
    real_k = real_z * kernel
    imag_k = imag_z * kernel
    back_real = along(cos_z, real_k, form_z) - along(sin_z, imag_k, form_z)
    back_imag = along(cos_z, imag_k, form_z) + along(sin_z, real_k, form_z)
    return jnp.stack([back_real, back_imag])


def solve_hartree(net, depth):
    planes, rows, cols = net.shape
    cos_x, sin_x = tables(cols)
    cos_y, sin_y = tables(rows)
    cos_z, sin_z = tables(depth)
    local_rows = rows // lax.axis_size("grid")
    row_index = lax.axis_index("grid") * local_rows + jnp.arange(local_rows, dtype=jnp.int32)
    real_x = jnp.dot(net, cos_x, precision=highest)
    imag_x = -jnp.dot(net, sin_x, precision=highest)
    real_y, imag_y = forward_y(cos_y, sin_y, real_x, imag_x)
    moved = lax.all_to_all(
        jnp.stack([real_y, imag_y]), "grid", split_axis=2, concat_axis=1, tiled=True
    )
    kernel = kernel_at(depth, row_index, rows, jnp.arange(cols, dtype=jnp.int32), cols)
    back = z_kernel(cos_z, sin_z, moved, kernel)
    returned = lax.all_to_all(back, "grid", split_axis=1, concat_axis=2, tiled=True)
    plane_real, plane_imag = inverse_y(cos_y, sin_y, returned[0], returned[1])
    result = jnp.dot(plane_real, cos_x, precision=highest) - jnp.dot(
        plane_imag, sin_x, precision=highest
    )
    return result / (cols * rows * depth)


def local(ng, orbitals, occupation, spin_of_band, ionic_charge):
    bands, planes, rows, cols = orbitals.shape
    total = bands * lax.axis_size("band")
    channels = jnp.arange(2, dtype=jnp.int32)
    weights = (
        jnp.where(
            spin_of_band[None, :] == channels[:, None], occupation[None, :].astype(jnp.float32), 0.0
        )
        / total
    )
    values = orbitals.astype(jnp.float32)
    squares = (values * values).reshape(bands, -1)
    partial_value = jnp.dot(weights, squares, precision=highest).reshape(2, planes, rows, cols)
    share = lax.psum_scatter(partial_value, "band", scatter_dimension=2, tiled=True)
    share_rows = share.shape[2]
    ion_share = lax.dynamic_slice_in_dim(
        ionic_charge, lax.axis_index("band") * share_rows, share_rows, 1
    )
    fields = jnp.concatenate(
        [-jnp.cbrt(6.0 / math.pi * share), (share[0] + share[1] - ion_share)[None]], 0
    )
    whole = lax.all_gather(fields, "band", axis=2, tiled=True)
    potential = solve_hartree(whole[2], planes * ng)[None] + whole[:2]
    pick = (spin_of_band[:, None] == channels[None, :]).astype(jnp.float32)
    chosen = jnp.dot(pick, potential.reshape(2, -1), precision=highest).reshape(
        bands, planes, rows, cols
    )
    applied = (chosen * values).astype(jnp.bfloat16)
    return (potential, applied)

MESH = pl.DeviceIdType.MESH
f32 = jnp.float32
bf16 = jnp.bfloat16


def cas_table(count):
    product = np.outer(np.arange(count), np.arange(count)) % count
    angle = 2.0 * math.pi * product / count
    return (np.cos(angle) + np.sin(angle)) / math.sqrt(count)


def parts_of(table):
    high = table.astype(np.float32).astype(bf16)
    low = (table - high.astype(np.float64)).astype(np.float32).astype(bf16)
    return high, low


def right_table(count):
    high, low = parts_of(cas_table(count))
    return np.concatenate([high, high, low], 0)


def left_table(count):
    high, low = parts_of(cas_table(count))
    return np.concatenate([high, low, high], 1)


def two_parts(value):
    high = value.astype(bf16)
    low = (value - high.astype(f32)).astype(bf16)
    return high, low


def right_mul(value, table):
    high, low = two_parts(value)
    return jnp.dot(jnp.concatenate([high, low, high], 1), table, preferred_element_type=f32)


def left_mul(table, value):
    high, low = two_parts(value)
    return jnp.dot(table, jnp.concatenate([high, high, low], 0), preferred_element_type=f32)


def cube_root(value):
    safe = jnp.where(value > 0, value, 1.0)
    return jnp.where(value > 0, jnp.exp(jnp.log(safe) * (1.0 / 3.0)), 0.0)


def wave_sq(index, count):
    signed = jnp.where(index < count // 2, index, index - count).astype(f32)
    wave = signed * (2.0 * math.pi / (count * spacing))
    return wave * wave


def field_kernel(
    ng, nb, lag,
    occ_hbm, spin_hbm, orb_hbm, ion_hbm, hx_hbm, hy_hbm, hz_hbm,
    pot, applied,
    occ, spin, orb, ion, hx, hy, hz, ex,
    part_a, near_in_a, near_out_a, far_in_a, far_out_a,
    part_b, near_in_b, near_out_b, far_in_b, far_out_b,
    y_out, z_in, z_out, y_in,
    orb_sem, in_sem, near_s, near_r, far_s, far_r, fwd_s, fwd_r, back_s, back_r,
):
    bands, planes, rows, cols = orb.shape
    depth = planes * ng
    lines = rows // ng
    group = 2
    g = lax.axis_index("grid")
    i = lax.axis_index("band")
    side = (2 * i) // nb
    inner = jnp.logical_and(i > 0, i < nb - 1)
    outer = jnp.logical_not(inner)
    inward = i + 1 - 2 * side
    outward = jnp.clip(i - 1 + 2 * side, 0, nb - 1)
    middle = jnp.where(side == 0, i + 1 == nb // 2, i == nb // 2)

    barrier = pltpu.get_barrier_semaphore()
    for k in range(1, ng):
        pl.semaphore_signal(barrier, inc=1, device_id={"grid": lax.rem(g + k, ng)}, device_id_type=MESH)
    pl.semaphore_signal(barrier, inc=1, device_id={"band": inward}, device_id_type=MESH)

    @pl.when(inner)
    def _():
        pl.semaphore_signal(barrier, inc=1, device_id={"band": outward}, device_id_type=MESH)

    moves = [(occ_hbm, occ), (spin_hbm, spin)]
    moves += [(ion_hbm, ion), (hx_hbm, hx), (hy_hbm, hy), (hz_hbm, hz)]
    others = [pltpu.make_async_copy(src, dst, in_sem.at[k]) for k, (src, dst) in enumerate(moves)]
    loads = [pltpu.make_async_copy(orb_hbm.at[:, p], orb.at[:, p], orb_sem.at[p]) for p in range(planes)]
    for copy in others[:2] + loads + others[2:]:
        copy.start()
    for copy in others[:2]:
        copy.wait()

    scale = 1.0 / (bands * nb)
    share = [spin[b].astype(f32) for b in range(bands)]
    up = [occ[b].astype(f32) * share[b] * scale for b in range(bands)]
    down = [occ[b].astype(f32) * (1.0 - share[b]) * scale for b in range(bands)]

    chain_a = (0, part_a, near_in_a, near_out_a, far_in_a, far_out_a)
    chain_b = (1, part_b, near_in_b, near_out_b, far_in_b, far_out_b)

    def inward_copy(chain, p, landing):
        n = chain[0]
        return pltpu.make_async_remote_copy(
            src_ref=chain[3].at[p], dst_ref=(chain[4] if landing else chain[2]).at[p],
            send_sem=near_s.at[n, p], recv_sem=(far_r if landing else near_r).at[n, p],
            device_id={"band": inward}, device_id_type=MESH,
        )

    def far_copy(chain, p):
        n = chain[0]
        return pltpu.make_async_remote_copy(
            src_ref=chain[5].at[p], dst_ref=chain[4].at[p],
            send_sem=far_s.at[n, p], recv_sem=far_r.at[n, p],
            device_id={"band": outward}, device_id_type=MESH,
        )

    def send_near(chain, p):
        @pl.when(middle)
        def _():
            inward_copy(chain, p, True).start()

        @pl.when(jnp.logical_not(middle))
        def _():
            inward_copy(chain, p, False).start()

    def near_step(chain, p):
        @pl.when(inner)
        def _():
            inward_copy(chain, p, False).wait_recv()
            chain[3][p] = chain[1][p] + chain[2][p]
            send_near(chain, p)

    def far_step(chain, p):
        far_copy(chain, p).wait_recv()

        @pl.when(inner)
        def _():
            chain[5][p] = chain[1][p] + chain[4][p]
            far_copy(chain, p).start()

    def fwd_copy(p, k):
        target = lax.rem(g + k, ng)
        return pltpu.make_async_remote_copy(
            src_ref=y_out.at[target, pl.ds(p * lines, group * lines)],
            dst_ref=z_in.at[pl.ds(pl.multiple_of((g * planes + p) * lines, group * lines), group * lines)],
            send_sem=fwd_s.at[p // group, k], recv_sem=fwd_r.at[p // group, k],
            device_id={"grid": target}, device_id_type=MESH,
        )

    def back_copy(start, k):
        target = lax.rem(g + k, ng)
        return pltpu.make_async_remote_copy(
            src_ref=z_out.at[target, pl.ds(start * planes, group * planes)],
            dst_ref=y_in.at[pl.ds(pl.multiple_of((g * lines + start) * planes, group * planes), group * planes)],
            send_sem=back_s.at[start // group, k], recv_sem=back_r.at[start // group, k],
            device_id={"grid": target}, device_id_type=MESH,
        )

    def forward(p):
        net = jnp.concatenate([near_out_a[q] + far_in_a[q] - ion[q] for q in (p, p + 1)], 0)
        mixed = right_mul(net, hx[...])
        spectrum = left_mul(hy[...], jnp.concatenate([mixed[:rows], mixed[rows:]], 1))
        for q in range(group):
            for t in range(ng):
                y_out[t, pl.ds((p + q) * lines, lines)] = spectrum[
                    t * lines:(t + 1) * lines, q * cols:(q + 1) * cols
                ]
        for k in range(1, ng):
            fwd_copy(p, k).start()
        z_in[pl.ds(pl.multiple_of((g * planes + p) * lines, group * lines), group * lines)] = y_out[
            g, pl.ds(p * lines, group * lines)
        ]

    def exchange(p):
        ex[p] = -cube_root((near_out_b[p] + far_in_b[p]) * (6.0 / math.pi))

    def finish(p):
        zero = pot[0, p] + ex[p, 0]
        one = pot[1, p] + ex[p, 1]
        pot[0, p] = zero
        pot[1, p] = one
        for b in range(bands):
            chosen = zero * (1.0 - share[b]) + one * share[b]
            applied[b, p] = (chosen * orb[b, p].astype(f32)).astype(bf16)

    for p in range(planes):
        loads[p].wait()
        zero = one = None
        for b in range(bands):
            value = orb[b, p].astype(f32)
            square = value * value
            zero = down[b] * square if b == 0 else zero + down[b] * square
            one = up[b] * square if b == 0 else one + up[b] * square
        both = zero + one

        @pl.when(inner)
        def _():
            part_a[p] = both
            part_b[p, 0] = zero
            part_b[p, 1] = one

        @pl.when(outer)
        def _():
            near_out_a[p] = both
            near_out_b[p, 0] = zero
            near_out_b[p, 1] = one

        if p == 0:
            pl.semaphore_wait(barrier, ng + jnp.where(inner, 1, 0))

        @pl.when(outer)
        def _():
            send_near(chain_a, p)

    @pl.when(outer)
    def _():
        for p in range(planes):
            send_near(chain_b, p)

    for copy in others[2:]:
        copy.wait()
    for step in range(planes + lag):
        if step < planes:
            near_step(chain_a, step)
        if step == planes + lag - 1:
            near_step(chain_b, 0)
        p = step - lag
        if p >= 0:
            far_step(chain_a, p)
            if p % group == group - 1:
                forward(p - group + 1)

    near_step(chain_b, 1)
    near_step(chain_b, 2)
    far_step(chain_b, 0)

    kz = lax.broadcasted_iota(jnp.int32, (depth, cols), 0)
    kx = lax.broadcasted_iota(jnp.int32, (depth, cols), 1)
    flat = wave_sq(kz, depth) + wave_sq(kx, cols)

    def kernel_of(line):
        total = flat + wave_sq(g * lines + line, rows)
        return jnp.where(total > 0, 4.0 * math.pi / jnp.where(total > 0, total, 1.0), 0.0)

    for p in range(0, planes, group):
        for k in range(1, ng):
            fwd_copy(p, k).wait_recv()
    for start in range(0, lines, group):
        picked = [z_in[pl.ds(start + t, depth, stride=lines), :] for t in range(group)]
        weights = jnp.concatenate([kernel_of(start + t) for t in range(group)], 1)
        waves = left_mul(hz[...], jnp.concatenate(picked, 1))
        field = left_mul(hz[...], waves * weights)
        for t in range(group):
            for d in range(ng):
                z_out[d, pl.ds((start + t) * planes, planes)] = field[
                    d * planes:(d + 1) * planes, t * cols:(t + 1) * cols
                ]
        for k in range(1, ng):
            back_copy(start, k).start()
        y_in[pl.ds(pl.multiple_of((g * lines + start) * planes, group * planes), group * planes)] = z_out[
            g, pl.ds(start * planes, group * planes)
        ]

    exchange(0)
    for step in range(3, planes):
        near_step(chain_b, step)
        far_step(chain_b, step - 2)
        exchange(step - 2)

    for start in range(0, lines, group):
        for k in range(1, ng):
            back_copy(start, k).wait_recv()
    for p in range(0, planes, group):
        picked = [y_in[pl.ds(p + t, rows, stride=planes), :] for t in range(group)]
        mixed = left_mul(hy[...], jnp.concatenate(picked, 1))
        both = right_mul(jnp.concatenate([mixed[:, :cols], mixed[:, cols:]], 0), hx[...])
        for t in range(group):
            hartree = both[t * rows:(t + 1) * rows]
            pot[0, p + t] = hartree
            pot[1, p + t] = hartree
    far_step(chain_b, planes - 2)
    for p in range(planes - 2):
        finish(p)
    exchange(planes - 2)
    finish(planes - 2)
    far_step(chain_b, planes - 1)
    exchange(planes - 1)
    finish(planes - 1)

    for p in range(planes):
        for chain in (chain_a, chain_b):
            inward_copy(chain, p, False).wait_send()

    @pl.when(inner)
    def _():
        for p in range(planes):
            for chain in (chain_a, chain_b):
                far_copy(chain, p).wait_send()

    for p in range(0, planes, group):
        for k in range(1, ng):
            fwd_copy(p, k).wait_send()
    for start in range(0, lines, group):
        for k in range(1, ng):
            back_copy(start, k).wait_send()


def fast(ng, nb, orbitals, occupation, spin_of_band, ionic_charge):
    bands, planes, rows, cols = orbitals.shape
    depth = planes * ng
    lines = rows // ng
    lag = 3
    dma = pltpu.SemaphoreType.DMA
    one = (planes, rows, cols)
    two = (planes, 2, rows, cols)
    return pl.pallas_call(
        functools.partial(field_kernel, ng, nb, lag),
        name="fields",
        out_shape=(
            jax.ShapeDtypeStruct((2, planes, rows, cols), f32),
            jax.ShapeDtypeStruct(orbitals.shape, bf16),
        ),
        in_specs=[pl.BlockSpec(memory_space=pltpu.HBM)] * 7,
        out_specs=(pl.BlockSpec(memory_space=pltpu.VMEM), pl.BlockSpec(memory_space=pltpu.VMEM)),
        scratch_shapes=[
            pltpu.SMEM((bands,), jnp.int32),
            pltpu.SMEM((bands,), jnp.int32),
            pltpu.VMEM(orbitals.shape, bf16),
            pltpu.VMEM(one, f32),
            pltpu.VMEM((3 * cols, cols), bf16),
            pltpu.VMEM((rows, 3 * rows), bf16),
            pltpu.VMEM((depth, 3 * depth), bf16),
            pltpu.VMEM(two, f32),
        ]
        + [pltpu.VMEM(one, f32)] * 5
        + [pltpu.VMEM(two, f32)] * 5
        + [
            pltpu.VMEM((ng, planes * lines, cols), f32),
            pltpu.VMEM((depth * lines, cols), f32),
            pltpu.VMEM((ng, planes * lines, cols), f32),
            pltpu.VMEM((rows * planes, cols), f32),
            dma((planes,)),
            dma((6,)),
            dma((2, planes)),
            dma((2, planes)),
            dma((2, planes)),
            dma((2, planes)),
            dma((planes // 2, ng)),
            dma((planes // 2, ng)),
            dma((lines // 2, ng)),
            dma((lines // 2, ng)),
        ],
        compiler_params=pltpu.CompilerParams(
            collective_id=0, has_side_effects=True, vmem_limit_bytes=32 * 1024 * 1024
        ),
    )(
        *(pltpu.with_memory_space_constraint(x, pltpu.HBM) for x in (
        occupation, spin_of_band, orbitals, ionic_charge,
        jnp.asarray(right_table(cols)), jnp.asarray(left_table(rows)), jnp.asarray(left_table(depth)),
    )))


def solution(mesh):
    ng, nb = mesh.shape["grid"], mesh.shape["band"]

    def body(orbitals, occupation, spin_of_band, ionic_charge):
        bands, planes, rows, cols = orbitals.shape
        lines = rows // ng
        suits = planes % 8 == 0 and lines % 8 == 0 and rows % 16 == 0
        if suits and cols % 128 == 0 and nb % 2 == 0 and ng > 1:
            return fast(ng, nb, orbitals, occupation, spin_of_band, ionic_charge)
        return local(ng, orbitals, occupation, spin_of_band, ionic_charge)

    return jax.shard_map(
        body,
        mesh=mesh,
        in_specs=(P("band", "grid", None, None), P("band"), P("band"), P("grid", None, None)),
        out_specs=(P(None, "grid", None, None), P("band", "grid", None, None)),
        check_vma=False,
    )
```

```python
import functools
import math

import jax
import jax.numpy as jnp
import numpy as np
from jax import lax
from jax.experimental import pallas as pl
from jax.experimental.pallas import tpu as pltpu
from jax.sharding import PartitionSpec as P

spacing = 0.25
highest = lax.Precision.HIGHEST


def tables(count):
    index = jnp.arange(count, dtype=jnp.int32)
    product = index[:, None] * index[None, :] % count
    angle = 2.0 * math.pi * product.astype(jnp.float32) / count
    return (jnp.cos(angle), jnp.sin(angle))


def signed_sq(index, count):
    signed = jnp.where(index < count // 2, index, index - count).astype(jnp.float32)
    wave = 2.0 * math.pi * signed / (count * spacing)
    return wave * wave


def kernel_at(depth, row_index, rows, col_index, cols):
    g_sq = signed_sq(jnp.arange(depth, dtype=jnp.int32), depth)[:, None, None]
    g_sq = g_sq + signed_sq(row_index, rows)[None, :, None]
    g_sq = g_sq + signed_sq(col_index, cols)[None, None, :]
    return jnp.where(g_sq > 0, 4.0 * math.pi / jnp.where(g_sq > 0, g_sq, 1.0), 0.0)


def along(table, field, form):
    return jnp.einsum(form, table, field, precision=highest)


def forward_y(cos_y, sin_y, real_x, imag_x):
    form_y = "ky,zyx->zkx"
    real_y = along(cos_y, real_x, form_y) + along(sin_y, imag_x, form_y)
    imag_y = along(cos_y, imag_x, form_y) - along(sin_y, real_x, form_y)
    return (real_y, imag_y)


def inverse_y(cos_y, sin_y, real_k, imag_k):
    form_y = "ky,zyx->zkx"
    plane_real = along(cos_y, real_k, form_y) - along(sin_y, imag_k, form_y)
    plane_imag = along(cos_y, imag_k, form_y) + along(sin_y, real_k, form_y)
    return (plane_real, plane_imag)


def z_kernel(cos_z, sin_z, moved, kernel):
    form_z = "kz,zyx->kyx"
    real_z = along(cos_z, moved[0], form_z) + along(sin_z, moved[1], form_z)
    imag_z = along(cos_z, moved[1], form_z) - along(sin_z, moved[0], form_z)
    real_k = real_z * kernel
    imag_k = imag_z * kernel
    back_real = along(cos_z, real_k, form_z) - along(sin_z, imag_k, form_z)
    back_imag = along(cos_z, imag_k, form_z) + along(sin_z, real_k, form_z)
    return jnp.stack([back_real, back_imag])


def solve_hartree(net, depth):
    planes, rows, cols = net.shape
    cos_x, sin_x = tables(cols)
    cos_y, sin_y = tables(rows)
    cos_z, sin_z = tables(depth)
    local_rows = rows // lax.axis_size("grid")
    row_index = lax.axis_index("grid") * local_rows + jnp.arange(local_rows, dtype=jnp.int32)
    real_x = jnp.dot(net, cos_x, precision=highest)
    imag_x = -jnp.dot(net, sin_x, precision=highest)
    real_y, imag_y = forward_y(cos_y, sin_y, real_x, imag_x)
    moved = lax.all_to_all(
        jnp.stack([real_y, imag_y]), "grid", split_axis=2, concat_axis=1, tiled=True
    )
    kernel = kernel_at(depth, row_index, rows, jnp.arange(cols, dtype=jnp.int32), cols)
    back = z_kernel(cos_z, sin_z, moved, kernel)
    returned = lax.all_to_all(back, "grid", split_axis=1, concat_axis=2, tiled=True)
    plane_real, plane_imag = inverse_y(cos_y, sin_y, returned[0], returned[1])
    result = jnp.dot(plane_real, cos_x, precision=highest) - jnp.dot(
        plane_imag, sin_x, precision=highest
    )
    return result / (cols * rows * depth)


def local(ng, orbitals, occupation, spin_of_band, ionic_charge):
    bands, planes, rows, cols = orbitals.shape
    total = bands * lax.axis_size("band")
    channels = jnp.arange(2, dtype=jnp.int32)
    weights = (
        jnp.where(
            spin_of_band[None, :] == channels[:, None], occupation[None, :].astype(jnp.float32), 0.0
        )
        / total
    )
    values = orbitals.astype(jnp.float32)
    squares = (values * values).reshape(bands, -1)
    partial_value = jnp.dot(weights, squares, precision=highest).reshape(2, planes, rows, cols)
    share = lax.psum_scatter(partial_value, "band", scatter_dimension=2, tiled=True)
    share_rows = share.shape[2]
    ion_share = lax.dynamic_slice_in_dim(
        ionic_charge, lax.axis_index("band") * share_rows, share_rows, 1
    )
    fields = jnp.concatenate(
        [-jnp.cbrt(6.0 / math.pi * share), (share[0] + share[1] - ion_share)[None]], 0
    )
    whole = lax.all_gather(fields, "band", axis=2, tiled=True)
    potential = solve_hartree(whole[2], planes * ng)[None] + whole[:2]
    pick = (spin_of_band[:, None] == channels[None, :]).astype(jnp.float32)
    chosen = jnp.dot(pick, potential.reshape(2, -1), precision=highest).reshape(
        bands, planes, rows, cols
    )
    applied = (chosen * values).astype(jnp.bfloat16)
    return (potential, applied)

MESH = pl.DeviceIdType.MESH
f32 = jnp.float32
bf16 = jnp.bfloat16


def cas_table(count):
    product = np.outer(np.arange(count), np.arange(count)) % count
    angle = 2.0 * math.pi * product / count
    return (np.cos(angle) + np.sin(angle)) / math.sqrt(count)


def parts_of(table):
    high = table.astype(np.float32).astype(bf16)
    low = (table - high.astype(np.float64)).astype(np.float32).astype(bf16)
    return high, low


def right_table(count):
    high, low = parts_of(cas_table(count))
    return np.concatenate([high, high, low], 0)


def left_table(count):
    high, low = parts_of(cas_table(count))
    return np.concatenate([high, low, high], 1)


def two_parts(value):
    high = value.astype(bf16)
    low = (value - high.astype(f32)).astype(bf16)
    return high, low


def right_mul(value, table):
    high, low = two_parts(value)
    return jnp.dot(jnp.concatenate([high, low, high], 1), table, preferred_element_type=f32)


def left_mul(table, value):
    high, low = two_parts(value)
    return jnp.dot(table, jnp.concatenate([high, high, low], 0), preferred_element_type=f32)


def cube_root(value):
    safe = jnp.where(value > 0, value, 1.0)
    return jnp.where(value > 0, jnp.exp(jnp.log(safe) * (1.0 / 3.0)), 0.0)


def wave_sq(index, count):
    signed = jnp.where(index < count // 2, index, index - count).astype(f32)
    wave = signed * (2.0 * math.pi / (count * spacing))
    return wave * wave


def field_kernel(
    ng, nb, lag, delay,
    occ_hbm, spin_hbm, orb_hbm, ion_hbm, hx_hbm, hy_hbm, hz_hbm,
    pot, applied,
    occ, spin, orb, ion, hx, hy, hz, ex,
    part_a, near_in_a, near_out_a, far_in_a, far_out_a,
    part_b, near_in_b, near_out_b, far_in_b, far_out_b,
    y_out, z_in, z_out, y_in,
    orb_sem, in_sem, near_s, near_r, far_s, far_r, fwd_s, fwd_r, back_s, back_r,
):
    bands, planes, rows, cols = orb.shape
    depth = planes * ng
    lines = rows // ng
    group = 2
    g = lax.axis_index("grid")
    i = lax.axis_index("band")
    side = (2 * i) // nb
    inner = jnp.logical_and(i > 0, i < nb - 1)
    outer = jnp.logical_not(inner)
    inward = i + 1 - 2 * side
    outward = jnp.clip(i - 1 + 2 * side, 0, nb - 1)
    middle = jnp.where(side == 0, i + 1 == nb // 2, i == nb // 2)

    barrier = pltpu.get_barrier_semaphore()
    for k in range(1, ng):
        pl.semaphore_signal(barrier, inc=1, device_id={"grid": lax.rem(g + k, ng)}, device_id_type=MESH)
    pl.semaphore_signal(barrier, inc=1, device_id={"band": inward}, device_id_type=MESH)

    @pl.when(inner)
    def _():
        pl.semaphore_signal(barrier, inc=1, device_id={"band": outward}, device_id_type=MESH)

    moves = [(occ_hbm, occ), (spin_hbm, spin)]
    moves += [(ion_hbm, ion), (hx_hbm, hx), (hy_hbm, hy), (hz_hbm, hz)]
    others = [pltpu.make_async_copy(src, dst, in_sem.at[k]) for k, (src, dst) in enumerate(moves)]
    loads = [pltpu.make_async_copy(orb_hbm.at[:, p], orb.at[:, p], orb_sem.at[p]) for p in range(planes)]
    for copy in others[:2] + loads + others[2:]:
        copy.start()
    for copy in others[:2]:
        copy.wait()

    scale = 1.0 / (bands * nb)
    share = [spin[b].astype(f32) for b in range(bands)]
    up = [occ[b].astype(f32) * share[b] * scale for b in range(bands)]
    down = [occ[b].astype(f32) * (1.0 - share[b]) * scale for b in range(bands)]

    chain_a = (0, part_a, near_in_a, near_out_a, far_in_a, far_out_a)
    chain_b = (1, part_b, near_in_b, near_out_b, far_in_b, far_out_b)

    def inward_copy(chain, p, landing):
        n = chain[0]
        return pltpu.make_async_remote_copy(
            src_ref=chain[3].at[p], dst_ref=(chain[4] if landing else chain[2]).at[p],
            send_sem=near_s.at[n, p], recv_sem=(far_r if landing else near_r).at[n, p],
            device_id={"band": inward}, device_id_type=MESH,
        )

    def far_copy(chain, p):
        n = chain[0]
        return pltpu.make_async_remote_copy(
            src_ref=chain[5].at[p], dst_ref=chain[4].at[p],
            send_sem=far_s.at[n, p], recv_sem=far_r.at[n, p],
            device_id={"band": outward}, device_id_type=MESH,
        )

    def send_near(chain, p):
        @pl.when(middle)
        def _():
            inward_copy(chain, p, True).start()

        @pl.when(jnp.logical_not(middle))
        def _():
            inward_copy(chain, p, False).start()

    def near_step(chain, p):
        @pl.when(inner)
        def _():
            inward_copy(chain, p, False).wait_recv()
            chain[3][p] = chain[1][p] + chain[2][p]
            send_near(chain, p)

    def far_step(chain, p):
        far_copy(chain, p).wait_recv()

        @pl.when(inner)
        def _():
            chain[5][p] = chain[1][p] + chain[4][p]
            far_copy(chain, p).start()

    def fwd_copy(p, k):
        target = lax.rem(g + k, ng)
        return pltpu.make_async_remote_copy(
            src_ref=y_out.at[target, pl.ds(p * lines, group * lines)],
            dst_ref=z_in.at[pl.ds(pl.multiple_of((g * planes + p) * lines, group * lines), group * lines)],
            send_sem=fwd_s.at[p // group, k], recv_sem=fwd_r.at[p // group, k],
            device_id={"grid": target}, device_id_type=MESH,
        )

    def back_copy(start, k):
        target = lax.rem(g + k, ng)
        return pltpu.make_async_remote_copy(
            src_ref=z_out.at[target, pl.ds(start * planes, group * planes)],
            dst_ref=y_in.at[pl.ds(pl.multiple_of((g * lines + start) * planes, group * planes), group * planes)],
            send_sem=back_s.at[start // group, k], recv_sem=back_r.at[start // group, k],
            device_id={"grid": target}, device_id_type=MESH,
        )

    def forward(p):
        net = jnp.concatenate([near_out_a[q] + far_in_a[q] - ion[q] for q in (p, p + 1)], 0)
        mixed = right_mul(net, hx[...])
        spectrum = left_mul(hy[...], jnp.concatenate([mixed[:rows], mixed[rows:]], 1))
        for q in range(group):
            for t in range(ng):
                y_out[t, pl.ds((p + q) * lines, lines)] = spectrum[
                    t * lines:(t + 1) * lines, q * cols:(q + 1) * cols
                ]
        for k in range(1, ng):
            fwd_copy(p, k).start()
        z_in[pl.ds(pl.multiple_of((g * planes + p) * lines, group * lines), group * lines)] = y_out[
            g, pl.ds(p * lines, group * lines)
        ]

    def exchange(p):
        ex[p] = -cube_root((near_out_b[p] + far_in_b[p]) * (6.0 / math.pi))

    def finish(p):
        zero = pot[0, p] + ex[p, 0]
        one = pot[1, p] + ex[p, 1]
        pot[0, p] = zero
        pot[1, p] = one
        for b in range(bands):
            chosen = zero * (1.0 - share[b]) + one * share[b]
            applied[b, p] = (chosen * orb[b, p].astype(f32)).astype(bf16)

    for p in range(planes):
        loads[p].wait()
        zero = one = None
        for b in range(bands):
            value = orb[b, p].astype(f32)
            square = value * value
            zero = down[b] * square if b == 0 else zero + down[b] * square
            one = up[b] * square if b == 0 else one + up[b] * square
        both = zero + one

        @pl.when(inner)
        def _():
            part_a[p] = both
            part_b[p, 0] = zero
            part_b[p, 1] = one

        @pl.when(outer)
        def _():
            near_out_a[p] = both
            near_out_b[p, 0] = zero
            near_out_b[p, 1] = one

        if p == 0:
            pl.semaphore_wait(barrier, ng + jnp.where(inner, 1, 0))

        @pl.when(outer)
        def _():
            send_near(chain_a, p)

    @pl.when(outer)
    def _():
        for p in range(planes):
            send_near(chain_b, p)

    for copy in others[2:]:
        copy.wait()
    for step in range(planes + lag):
        if step < planes:
            near_step(chain_a, step)
        if step == planes + lag - 1:
            near_step(chain_b, 0)
        p = step - lag
        if p >= 0:
            far_step(chain_a, p)
            if p % group == group - 1:
                forward(p - group + 1)

    for p in range(1, delay + 1):
        near_step(chain_b, p)
    far_step(chain_b, 0)

    kz = lax.broadcasted_iota(jnp.int32, (depth, cols), 0)
    kx = lax.broadcasted_iota(jnp.int32, (depth, cols), 1)
    flat = wave_sq(kz, depth) + wave_sq(kx, cols)

    def kernel_of(line):
        total = flat + wave_sq(g * lines + line, rows)
        return jnp.where(total > 0, 4.0 * math.pi / jnp.where(total > 0, total, 1.0), 0.0)

    for p in range(0, planes, group):
        for k in range(1, ng):
            fwd_copy(p, k).wait_recv()
    for start in range(0, lines, group):
        picked = [z_in[pl.ds(start + t, depth, stride=lines), :] for t in range(group)]
        weights = jnp.concatenate([kernel_of(start + t) for t in range(group)], 1)
        waves = left_mul(hz[...], jnp.concatenate(picked, 1))
        field = left_mul(hz[...], waves * weights)
        for t in range(group):
            for d in range(ng):
                z_out[d, pl.ds((start + t) * planes, planes)] = field[
                    d * planes:(d + 1) * planes, t * cols:(t + 1) * cols
                ]
        for k in range(1, ng):
            back_copy(start, k).start()
        y_in[pl.ds(pl.multiple_of((g * lines + start) * planes, group * planes), group * planes)] = z_out[
            g, pl.ds(start * planes, group * planes)
        ]

    exchange(0)
    for step in range(delay + 1, planes):
        near_step(chain_b, step)
        far_step(chain_b, step - delay)
        exchange(step - delay)

    for start in range(0, lines, group):
        for k in range(1, ng):
            back_copy(start, k).wait_recv()
    for p in range(0, planes, group):
        picked = [y_in[pl.ds(p + t, rows, stride=planes), :] for t in range(group)]
        mixed = left_mul(hy[...], jnp.concatenate(picked, 1))
        both = right_mul(jnp.concatenate([mixed[:, :cols], mixed[:, cols:]], 0), hx[...])
        for t in range(group):
            hartree = both[t * rows:(t + 1) * rows]
            pot[0, p + t] = hartree
            pot[1, p + t] = hartree
    for p in range(planes - delay, planes):
        far_step(chain_b, p)
        if p == planes - delay:
            for q in range(p):
                finish(q)
        exchange(p)
        finish(p)

    for p in range(planes):
        for chain in (chain_a, chain_b):
            inward_copy(chain, p, False).wait_send()

    @pl.when(inner)
    def _():
        for p in range(planes):
            for chain in (chain_a, chain_b):
                far_copy(chain, p).wait_send()

    for p in range(0, planes, group):
        for k in range(1, ng):
            fwd_copy(p, k).wait_send()
    for start in range(0, lines, group):
        for k in range(1, ng):
            back_copy(start, k).wait_send()


def fast(ng, nb, orbitals, occupation, spin_of_band, ionic_charge):
    bands, planes, rows, cols = orbitals.shape
    depth = planes * ng
    lines = rows // ng
    lag, delay = 4, 3
    dma = pltpu.SemaphoreType.DMA
    one = (planes, rows, cols)
    two = (planes, 2, rows, cols)
    return pl.pallas_call(
        functools.partial(field_kernel, ng, nb, lag, delay),
        name="fields",
        out_shape=(
            jax.ShapeDtypeStruct((2, planes, rows, cols), f32),
            jax.ShapeDtypeStruct(orbitals.shape, bf16),
        ),
        in_specs=[pl.BlockSpec(memory_space=pltpu.HBM)] * 7,
        out_specs=(pl.BlockSpec(memory_space=pltpu.VMEM), pl.BlockSpec(memory_space=pltpu.VMEM)),
        scratch_shapes=[
            pltpu.SMEM((bands,), jnp.int32),
            pltpu.SMEM((bands,), jnp.int32),
            pltpu.VMEM(orbitals.shape, bf16),
            pltpu.VMEM(one, f32),
            pltpu.VMEM((3 * cols, cols), bf16),
            pltpu.VMEM((rows, 3 * rows), bf16),
            pltpu.VMEM((depth, 3 * depth), bf16),
            pltpu.VMEM(two, f32),
        ]
        + [pltpu.VMEM(one, f32)] * 5
        + [pltpu.VMEM(two, f32)] * 5
        + [
            pltpu.VMEM((ng, planes * lines, cols), f32),
            pltpu.VMEM((depth * lines, cols), f32),
            pltpu.VMEM((ng, planes * lines, cols), f32),
            pltpu.VMEM((rows * planes, cols), f32),
            dma((planes,)),
            dma((6,)),
            dma((2, planes)),
            dma((2, planes)),
            dma((2, planes)),
            dma((2, planes)),
            dma((planes // 2, ng)),
            dma((planes // 2, ng)),
            dma((lines // 2, ng)),
            dma((lines // 2, ng)),
        ],
        compiler_params=pltpu.CompilerParams(
            collective_id=0, has_side_effects=True, vmem_limit_bytes=32 * 1024 * 1024
        ),
    )(
        *(pltpu.with_memory_space_constraint(x, pltpu.HBM) for x in (
        occupation, spin_of_band, orbitals, ionic_charge,
        jnp.asarray(right_table(cols)), jnp.asarray(left_table(rows)), jnp.asarray(left_table(depth)),
    )))


def solution(mesh):
    ng, nb = mesh.shape["grid"], mesh.shape["band"]

    def body(orbitals, occupation, spin_of_band, ionic_charge):
        bands, planes, rows, cols = orbitals.shape
        lines = rows // ng
        suits = planes % 8 == 0 and lines % 8 == 0 and rows % 16 == 0
        if suits and cols % 128 == 0 and nb % 2 == 0 and ng > 1:
            return fast(ng, nb, orbitals, occupation, spin_of_band, ionic_charge)
        return local(ng, orbitals, occupation, spin_of_band, ionic_charge)

    return jax.shard_map(
        body,
        mesh=mesh,
        in_specs=(P("band", "grid", None, None), P("band"), P("band"), P("grid", None, None)),
        out_specs=(P(None, "grid", None, None), P("band", "grid", None, None)),
        check_vma=False,
    )
```
